32 devices in a mesh: space: 2 (over x), energy: 16 (over z, y, core).
Axes of the slice: x: 2, y: 2, z: 4, core: 2. Of those that a mesh axis runs over, the one named last changes fastest.
Arguments:
- lesser_in: bfloat16 [16, 2, 2, 256, 256], P('energy', 'space'), may hold values from -6 to 6
- retarded: bfloat16 [16, 2, 2, 256, 256], P('energy', 'space'), may hold values from -0.25 to 0.25
- coupling: bfloat16 [2, 2, 256, 256], P('space'), may hold values from -0.25 to 0.25
- interaction: bfloat16 [2, 32, 65536], P('space', None, 'energy'), may hold values from -1.5 to 1.5
Outputs:
- self_energy: bfloat16 [16, 2, 2, 256, 256], P('energy', 'space')
The draws below stay inside these ranges and needn't reach their ends.
All inputs are finite; a program needn't handle non-finite values.
Results may differ from the reference program's by a relative error of at most 0.029.
Values may be sent and summed in bfloat16 or wider, within the bound.
A program may use at most 128 MiB of HBM per device.

```python
import math
import jax
import jax.numpy as jnp
from jax import lax

B = 256
NBLK = 2
NE = 16
NFFT = 32


def level_of(stream_key, extent, split, low, high):
    gain, own = 1.0, jax.random.fold_in(stream_key, 6)
    for axis_at, parts in split:
        heights = jnp.exp(jax.random.uniform(jax.random.fold_in(own, axis_at), (parts,), jnp.float32, low / len(split), high / len(split)))
        gain = gain * jnp.repeat(heights, extent[axis_at] // parts).reshape([-1 if axis == axis_at else 1 for axis in range(len(extent))])
    return gain


def normal_values(key, extent, width, reach, shards=(), kind=jnp.bfloat16):
    values = jax.random.normal(key, extent, jnp.float32) * width
    if len(shards) > 0:
        values = level_of(key, extent, shards, -0.22, 0.18) * values
    return jnp.clip(values, min=-reach, max=reach).astype(kind)


def setup_inputs(seed: int = 0) -> dict:
    key_list = jax.random.split(jax.random.key(seed), 5)
    lesser_in = normal_values(key_list[0], (NE, NBLK, 2, B, B), 1.0, 6.0, ((0, 16), (1, 2)))
    retarded = normal_values(key_list[1], (NE, NBLK, 2, B, B), (2 * B) ** -0.5, 0.25, ((0, 16), (1, 2)))
    coupling = normal_values(key_list[2], (NBLK, 2, B, B), (2 * B + B // 3) ** -0.5, 0.25, ((0, 2),))
    interaction = normal_values(key_list[3], (NBLK, NFFT, B * B), 0.25, 1.5, ((0, 2), (2, 16)))
    return dict(lesser_in=lesser_in, retarded=retarded, coupling=coupling, interaction=interaction)


def product(left_real, left_imag, right_real, right_imag):
    real_part = jnp.dot(left_real, right_real, preferred_element_type=jnp.float32) - jnp.dot(left_imag, right_imag, preferred_element_type=jnp.float32)
    imag_part = jnp.dot(left_real, right_imag, preferred_element_type=jnp.float32) + jnp.dot(left_imag, right_real, preferred_element_type=jnp.float32)
    return real_part, imag_part


def contract(former, latter):
    return lax.dot_general(former, latter, (((1,), (1,)), ((), ())), preferred_element_type=jnp.float32)


def product_adjoint(left_real, left_imag, right_real, right_imag):
    real_part = contract(left_real, right_real) + contract(left_imag, right_imag)
    imag_part = contract(left_imag, right_real) - contract(left_real, right_imag)
    return real_part, imag_part


def phase_table(row_count, column_count, length):
    row_index = jnp.arange(row_count, dtype=jnp.int32)[:, None]
    column_index = jnp.arange(column_count, dtype=jnp.int32)[None, :]
    residue = (row_index * column_index) % length
    return residue.astype(jnp.float32) * (2.0 * math.pi / length)


def finish(spectrum_real, spectrum_imag, weights, energy_count, length):
    forward_scale = energy_count ** -0.5
    inverse_scale = length ** -0.5
    spectrum_real = spectrum_real * forward_scale
    spectrum_imag = spectrum_imag * forward_scale
    weight_values = weights.astype(jnp.float32)
    squared_real = ((spectrum_real * spectrum_real - spectrum_imag * spectrum_imag) * weight_values).astype(jnp.bfloat16)
    squared_imag = (2.0 * spectrum_real * spectrum_imag * weight_values).astype(jnp.bfloat16)
    inverse_phase = phase_table(energy_count, length, length)
    inverse_real = jnp.cos(inverse_phase).astype(jnp.bfloat16)
    inverse_imag = jnp.sin(inverse_phase).astype(jnp.bfloat16)
    out_real, out_imag = product(inverse_real, inverse_imag, squared_real, squared_imag)
    return jnp.stack([out_real * inverse_scale, out_imag * inverse_scale], axis=1).astype(jnp.bfloat16)


def reference(lesser_in, retarded, coupling, interaction):
    block_order = coupling.shape[-1]
    block_count = coupling.shape[0]
    energy_count = lesser_in.shape[0]
    length = 2 * energy_count

    def one_energy(inputs_pair):
        green_in, lesser_here = inputs_pair
        carried_real = jnp.zeros((block_order, block_order), jnp.bfloat16)
        carried_imag = jnp.zeros((block_order, block_order), jnp.bfloat16)
        layers = []
        for block_index in range(block_count):
            resolvent_real = green_in[block_index, 0]
            resolvent_imag = green_in[block_index, 1]
            map_real, map_imag = product(resolvent_real, resolvent_imag, coupling[block_index, 0], coupling[block_index, 1])
            map_real = map_real.astype(jnp.bfloat16)
            map_imag = map_imag.astype(jnp.bfloat16)
            half_real, half_imag = product(resolvent_real, resolvent_imag, lesser_here[block_index, 0], lesser_here[block_index, 1])
            half_real = half_real.astype(jnp.bfloat16)
            half_imag = half_imag.astype(jnp.bfloat16)
            source_real, source_imag = product_adjoint(half_real, half_imag, resolvent_real, resolvent_imag)
            carry_real, carry_imag = product(map_real, map_imag, carried_real, carried_imag)
            carry_real = carry_real.astype(jnp.bfloat16)
            carry_imag = carry_imag.astype(jnp.bfloat16)
            grown_real, grown_imag = product_adjoint(carry_real, carry_imag, map_real, map_imag)
            carried_real = (source_real + grown_real).astype(jnp.bfloat16)
            carried_imag = (source_imag + grown_imag).astype(jnp.bfloat16)
            layers.append(jnp.stack([carried_real, carried_imag]))
        return jnp.stack(layers)

    green_lesser = lax.map(one_energy, (retarded, lesser_in))
    forward_phase = phase_table(length, energy_count, length)
    forward_real = jnp.cos(forward_phase).astype(jnp.bfloat16)
    forward_imag = (-jnp.sin(forward_phase)).astype(jnp.bfloat16)

    def one_block(inputs_pair):
        green_block, weights = inputs_pair
        flattened = green_block.reshape(energy_count, 2, block_order * block_order)
        spectrum_real, spectrum_imag = product(forward_real, forward_imag, flattened[:, 0], flattened[:, 1])
        result = finish(spectrum_real, spectrum_imag, weights, energy_count, length)
        return result.reshape(energy_count, 2, block_order, block_order)

    per_block = lax.map(one_block, (jnp.moveaxis(green_lesser, 1, 0), interaction))
    return jnp.moveaxis(per_block, 0, 1)
```

```python
import functools
import math

import jax
import jax.numpy as jnp
import numpy as np
from jax import lax
from jax.experimental import pallas as pl
from jax.experimental.pallas import tpu as pltpu
from jax.sharding import PartitionSpec as P

MESH = pl.DeviceIdType.MESH
ANY = pl.BlockSpec(memory_space=pl.ANY)


def phase_parts(row_count, column_count, length):
    residue = np.arange(row_count)[:, None] * np.arange(column_count)[None, :] % length
    phase = residue * (2.0 * math.pi / length)
    return np.cos(phase), np.sin(phase)


def forward_matrix(energy_count, length, rows):
    cosine, sine = phase_parts(length, energy_count, length)
    small = np.array([[cosine, sine], [-sine, cosine]])
    full = np.einsum("pqfe,rs->rpfeqs", small, np.eye(rows))
    return full.reshape(rows * 2 * length, energy_count * 2 * rows).astype(jnp.bfloat16)


def inverse_matrix(energy_count, length, rows):
    cosine, sine = phase_parts(energy_count, length, length)
    small = np.array([[cosine, -sine], [sine, cosine]])
    full = np.einsum("pqef,rs->eprsqf", small, np.eye(rows))
    return full.reshape(energy_count * 2 * rows, rows * 2 * length).astype(jnp.bfloat16)


def dot(left, right):
    return jnp.dot(left, right, preferred_element_type=jnp.float32)


def dot_t(left, right):
    return lax.dot_general(
        left, right, (((1,), (1,)), ((), ())), preferred_element_type=jnp.float32
    )


def kernel(
    sections, groups, rows, length, pieces,
    lesser_hbm, retarded_hbm, coupling_hbm, interaction_hbm, forward_hbm, inverse_hbm,
    out_hbm,
    lesser, retarded, coupling, interaction, forward, inverse,
    total, maps, green, before, homing, homed, weighted, leaving,
    load_sem, hop_send, hop_recv, go_send, go_recv, back_send, back_recv, own_sem,
):
    section = lax.axis_index("space")
    me = lax.axis_index("energy")
    order = green.shape[-1]
    width = order // pieces

    barrier = pltpu.get_barrier_semaphore()
    for step in range(1, groups):
        peer = lax.rem(me + step, groups)
        pl.semaphore_signal(barrier, inc=1, device_id={"energy": peer}, device_id_type=MESH)

    @pl.when(section > 0)
    def _():
        pl.semaphore_signal(barrier, inc=1, device_id={"space": section - 1}, device_id_type=MESH)

    @pl.when(section < sections - 1)
    def _():
        pl.semaphore_signal(barrier, inc=1, device_id={"space": section + 1}, device_id_type=MESH)

    loads = []
    for at, (source, target) in enumerate((
        (retarded_hbm.at[0, 0], retarded),
        (lesser_hbm.at[0, 0], lesser),
        (coupling_hbm.at[0], coupling),
        (interaction_hbm.at[0], interaction),
        (forward_hbm, forward),
        (inverse_hbm, inverse),
    )):
        load = pltpu.make_async_copy(source, target, load_sem.at[at])
        load.start()
        loads.append(load)

    loads[0].wait()
    loads[1].wait()
    r_re, r_im = retarded[0], retarded[1]
    l_re, l_im = lesser[0], lesser[1]
    half_re = (dot(r_re, l_re) - dot(r_im, l_im)).astype(jnp.bfloat16)
    half_im = (dot(r_re, l_im) + dot(r_im, l_re)).astype(jnp.bfloat16)
    total[0] = dot_t(half_re, r_re) + dot_t(half_im, r_im)
    total[1] = dot_t(half_im, r_re) - dot_t(half_re, r_im)

    pl.semaphore_wait(
        barrier,
        groups - 1 + jnp.where(section > 0, 1, 0) + jnp.where(section < sections - 1, 1, 0),
    )
    loads[2].wait()

    def hop(piece, target):
        columns = pl.ds(piece * width, width)
        return pltpu.make_async_remote_copy(
            src_ref=green.at[:, :, columns],
            dst_ref=before.at[:, :, columns],
            send_sem=hop_send.at[piece],
            recv_sem=hop_recv.at[piece],
            device_id={"space": target},
            device_id_type=MESH,
        )

    @pl.when(section > 0)
    def _():
        c_re, c_im = coupling[0], coupling[1]
        maps[0] = (dot(r_re, c_re) - dot(r_im, c_im)).astype(jnp.bfloat16)
        maps[1] = (dot(r_re, c_im) + dot(r_im, c_re)).astype(jnp.bfloat16)
        for piece in range(pieces):
            hop(piece, section - 1).wait_recv()
            part = slice(piece * width, (piece + 1) * width)
            b_re, b_im = before[0, :, part], before[1, :, part]
            m_re, m_im = maps[0], maps[1]
            k_re = (dot(m_re, b_re) - dot(m_im, b_im)).astype(jnp.bfloat16)
            k_im = (dot(m_re, b_im) + dot(m_im, b_re)).astype(jnp.bfloat16)
            n_re, n_im = maps[0, :, part], maps[1, :, part]
            total[0] += dot_t(k_re, n_re) + dot_t(k_im, n_im)
            total[1] += dot_t(k_im, n_re) - dot_t(k_re, n_im)

    @pl.when(section < sections - 1)
    def _():
        green[...] = total[...].astype(jnp.bfloat16)
        for piece in range(pieces):
            hop(piece, section + 1).start()

    homing[...] = jnp.concatenate(
        [total[part].reshape(groups, rows, order) for part in range(2)], axis=1
    ).astype(jnp.bfloat16)

    def go(peer, slot):
        return pltpu.make_async_remote_copy(
            src_ref=homing.at[peer],
            dst_ref=homed.at[slot],
            send_sem=go_send.at[peer],
            recv_sem=go_recv.at[slot],
            device_id={"energy": peer},
            device_id_type=MESH,
        )

    def back(peer, slot):
        return pltpu.make_async_remote_copy(
            src_ref=leaving.at[peer],
            dst_ref=out_hbm.at[slot],
            send_sem=back_send.at[peer],
            recv_sem=back_recv.at[slot],
            device_id={"energy": peer},
            device_id_type=MESH,
        )

    peers = [lax.rem(me + step, groups) for step in range(1, groups)]
    for peer in peers:
        go(peer, me).start()
    own = pltpu.make_async_copy(homing.at[me], homed.at[me], own_sem.at[0])
    own.start()
    for load in loads[3:]:
        load.wait()
    own.wait()
    for peer in peers:
        go(peer, peer).wait_recv()

    entries = homed[...]
    if 2 * rows % 16:
        entries = entries.astype(jnp.float32)
    entries = entries.reshape(groups * 2 * rows, order).astype(jnp.bfloat16)
    stride = 2 * length
    chunk = max(1, order // stride)
    for first in range(0, rows, chunk):
        spectrum = dot(forward[first * stride:(first + chunk) * stride, :], entries)
        spectrum = spectrum * groups ** -0.5
        for at in range(chunk):
            row = first + at
            s_re = spectrum[at * stride:at * stride + length]
            s_im = spectrum[at * stride + length:(at + 1) * stride]
            weight = interaction[:, row * order:(row + 1) * order].astype(jnp.float32)
            weighted[row * stride:row * stride + length, :] = (
                (s_re * s_re - s_im * s_im) * weight
            ).astype(jnp.bfloat16)
            weighted[row * stride + length:(row + 1) * stride, :] = (
                2.0 * s_re * s_im * weight
            ).astype(jnp.bfloat16)
    result = dot(inverse[...], weighted[...]) * length ** -0.5
    leaving[...] = result.reshape(groups, 2 * rows, order).astype(jnp.bfloat16)

    for peer in peers:
        back(peer, me).start()
    own = pltpu.make_async_copy(leaving.at[me], out_hbm.at[me], own_sem.at[1])
    own.start()
    for peer in peers:
        go(peer, me).wait_send()

    @pl.when(section < sections - 1)
    def _():
        for piece in range(pieces):
            hop(piece, section + 1).wait_send()

    own.wait()
    for peer in peers:
        back(peer, me).wait_send()
    for peer in peers:
        back(peer, peer).wait_recv()


def local(lesser_in, retarded, coupling, interaction):
    order = coupling.shape[-1]
    groups = lax.axis_size("energy")
    sections = lax.axis_size("space")
    length = interaction.shape[1]
    rows = order // groups
    pieces = 2
    assert lesser_in.shape[0] == 1 and coupling.shape[0] == 1
    forward = jnp.asarray(forward_matrix(groups, length, rows))
    inverse = jnp.asarray(inverse_matrix(groups, length, rows))
    low, wide = jnp.bfloat16, jnp.float32
    dma = pltpu.SemaphoreType.DMA
    returned = pl.pallas_call(
        functools.partial(kernel, sections, groups, rows, length, pieces),
        out_shape=jax.ShapeDtypeStruct((groups, 2 * rows, order), low),
        in_specs=[ANY] * 6,
        out_specs=ANY,
        scratch_shapes=[
            pltpu.VMEM((2, order, order), low),
            pltpu.VMEM((2, order, order), low),
            pltpu.VMEM((2, order, order), low),
            pltpu.VMEM(interaction.shape[1:], low),
            pltpu.VMEM(forward.shape, low),
            pltpu.VMEM(inverse.shape, low),
            pltpu.VMEM((2, order, order), wide),
            pltpu.VMEM((2, order, order), low),
            pltpu.VMEM((2, order, order), low),
            pltpu.VMEM((2, order, order), low),
            pltpu.VMEM((groups, 2 * rows, order), low),
            pltpu.VMEM((groups, 2 * rows, order), low),
            pltpu.VMEM((rows * 2 * length, order), low),
            pltpu.VMEM((groups, 2 * rows, order), low),
            dma((6,)),
            dma((pieces,)),
            dma((pieces,)),
            dma((groups,)),
            dma((groups,)),
            dma((groups,)),
            dma((groups,)),
            dma((2,)),
        ],
        compiler_params=pltpu.CompilerParams(
            collective_id=0, has_side_effects=True
        ),
    )(lesser_in, retarded, coupling, interaction, forward, inverse)
    returned = returned.reshape(groups, 2, rows, order).transpose(1, 0, 2, 3)
    return returned.reshape(1, 1, 2, order, order)


def solution(mesh):
    in_specs = (
        P("energy", "space", None, None, None),
        P("energy", "space", None, None, None),
        P("space", None, None, None),
        P("space", None, "energy"),
    )
    out_specs = P("energy", "space", None, None, None)
    return jax.shard_map(local, mesh=mesh, in_specs=in_specs, out_specs=out_specs, check_vma=False)
```

```python
import functools
import math

import jax
import jax.numpy as jnp
import numpy as np
from jax import lax
from jax.experimental import pallas as pl
from jax.experimental.pallas import tpu as pltpu
from jax.sharding import PartitionSpec as P

MESH = pl.DeviceIdType.MESH
ANY = pl.BlockSpec(memory_space=pl.ANY)


def phase_parts(row_count, column_count, length):
    residue = np.arange(row_count)[:, None] * np.arange(column_count)[None, :] % length
    phase = residue * (2.0 * math.pi / length)
    return np.cos(phase), np.sin(phase)


def forward_matrix(energy_count, length, rows):
    cosine, sine = phase_parts(length, energy_count, length)
    small = np.array([[cosine, sine], [-sine, cosine]])
    full = np.einsum("pqfe,rs->rpfeqs", small, np.eye(rows))
    return full.reshape(rows * 2 * length, energy_count * 2 * rows).astype(jnp.bfloat16)


def inverse_matrix(energy_count, length, rows):
    cosine, sine = phase_parts(energy_count, length, length)
    small = np.array([[cosine, -sine], [sine, cosine]])
    full = np.einsum("pqef,rs->eprsqf", small, np.eye(rows))
    return full.reshape(energy_count * 2 * rows, rows * 2 * length).astype(jnp.bfloat16)


def dot(left, right):
    return jnp.dot(left, right, preferred_element_type=jnp.float32)


def dot_t(left, right):
    return lax.dot_general(
        left, right, (((1,), (1,)), ((), ())), preferred_element_type=jnp.float32
    )


def kernel(
    sections, groups, rows, length, pieces, parts,
    lesser_hbm, retarded_hbm, coupling_hbm, interaction_hbm, forward_hbm, inverse_hbm,
    out_hbm,
    lesser, retarded, coupling, interaction, forward, inverse,
    total, maps, green, before, homing, homed, weighted, leaving,
    load_sem, hop_send, hop_recv, go_send, go_recv, back_send, back_recv, own_sem,
):
    section = lax.axis_index("space")
    me = lax.axis_index("energy")
    order = green.shape[-1]
    width = order // pieces

    barrier = pltpu.get_barrier_semaphore()
    for step in range(1, groups):
        peer = lax.rem(me + step, groups)
        pl.semaphore_signal(barrier, inc=1, device_id={"energy": peer}, device_id_type=MESH)

    @pl.when(section > 0)
    def _():
        pl.semaphore_signal(barrier, inc=1, device_id={"space": section - 1}, device_id_type=MESH)

    @pl.when(section < sections - 1)
    def _():
        pl.semaphore_signal(barrier, inc=1, device_id={"space": section + 1}, device_id_type=MESH)

    loads = []
    for at, (source, target) in enumerate((
        (retarded_hbm.at[0, 0], retarded),
        (lesser_hbm.at[0, 0], lesser),
        (coupling_hbm.at[0], coupling),
        (interaction_hbm.at[0], interaction),
        (forward_hbm, forward),
        (inverse_hbm, inverse),
    )):
        load = pltpu.make_async_copy(source, target, load_sem.at[at])
        load.start()
        loads.append(load)

    loads[0].wait()
    loads[1].wait()
    r_re, r_im = retarded[0], retarded[1]
    l_re, l_im = lesser[0], lesser[1]
    half_re = (dot(r_re, l_re) - dot(r_im, l_im)).astype(jnp.bfloat16)
    half_im = (dot(r_re, l_im) + dot(r_im, l_re)).astype(jnp.bfloat16)
    total[0] = dot_t(half_re, r_re) + dot_t(half_im, r_im)
    total[1] = dot_t(half_im, r_re) - dot_t(half_re, r_im)

    pl.semaphore_wait(
        barrier,
        groups - 1 + jnp.where(section > 0, 1, 0) + jnp.where(section < sections - 1, 1, 0),
    )
    loads[2].wait()

    def hop(piece, target):
        columns = pl.ds(piece * width, width)
        return pltpu.make_async_remote_copy(
            src_ref=green.at[:, :, columns],
            dst_ref=before.at[:, :, columns],
            send_sem=hop_send.at[piece],
            recv_sem=hop_recv.at[piece],
            device_id={"space": target},
            device_id_type=MESH,
        )

    @pl.when(section > 0)
    def _():
        c_re, c_im = coupling[0], coupling[1]
        maps[0] = (dot(r_re, c_re) - dot(r_im, c_im)).astype(jnp.bfloat16)
        maps[1] = (dot(r_re, c_im) + dot(r_im, c_re)).astype(jnp.bfloat16)
        for piece in range(pieces):
            hop(piece, section - 1).wait_recv()
            part = slice(piece * width, (piece + 1) * width)
            b_re, b_im = before[0, :, part], before[1, :, part]
            m_re, m_im = maps[0], maps[1]
            k_re = (dot(m_re, b_re) - dot(m_im, b_im)).astype(jnp.bfloat16)
            k_im = (dot(m_re, b_im) + dot(m_im, b_re)).astype(jnp.bfloat16)
            n_re, n_im = maps[0, :, part], maps[1, :, part]
            total[0] += dot_t(k_re, n_re) + dot_t(k_im, n_im)
            total[1] += dot_t(k_im, n_re) - dot_t(k_re, n_im)

    @pl.when(section < sections - 1)
    def _():
        green[...] = total[...].astype(jnp.bfloat16)
        for piece in range(pieces):
            hop(piece, section + 1).start()

    share = rows // parts
    for part in range(parts):
        homing[part] = jnp.concatenate(
            [
                total[side].reshape(groups, parts, share, order)[:, part]
                for side in range(2)
            ],
            axis=1,
        ).astype(jnp.bfloat16)

    def go(part, peer, slot):
        return pltpu.make_async_remote_copy(
            src_ref=homing.at[part, peer],
            dst_ref=homed.at[part, slot],
            send_sem=go_send.at[part, peer],
            recv_sem=go_recv.at[part, slot],
            device_id={"energy": peer},
            device_id_type=MESH,
        )

    def back(part, peer, slot):
        return pltpu.make_async_remote_copy(
            src_ref=leaving.at[part, peer],
            dst_ref=out_hbm.at[slot, part],
            send_sem=back_send.at[part, peer],
            recv_sem=back_recv.at[part, slot],
            device_id={"energy": peer},
            device_id_type=MESH,
        )

    peers = [lax.rem(me + step, groups) for step in range(1, groups)]
    kept = []
    for part in range(parts):
        for peer in peers:
            go(part, peer, me).start()
        own = pltpu.make_async_copy(homing.at[part, me], homed.at[part, me], own_sem.at[0, part])
        own.start()
        kept.append(own)
    for load in loads[3:]:
        load.wait()

    stride = 2 * length
    chunk = max(1, order // stride)
    returns = []
    for part in range(parts):
        kept[part].wait()
        for peer in peers:
            go(part, peer, peer).wait_recv()
        entries = homed[part]
        if 2 * share % 16:
            entries = entries.astype(jnp.float32)
        entries = entries.reshape(groups * 2 * share, order).astype(jnp.bfloat16)
        for first in range(0, share, chunk):
            spectrum = dot(forward[first * stride:(first + chunk) * stride, :], entries)
            spectrum = spectrum * groups ** -0.5
            for at in range(chunk):
                row = first + at
                s_re = spectrum[at * stride:at * stride + length]
                s_im = spectrum[at * stride + length:(at + 1) * stride]
                entry = (part * share + row) * order
                weight = interaction[:, entry:entry + order].astype(jnp.float32)
                weighted[row * stride:row * stride + length, :] = (
                    (s_re * s_re - s_im * s_im) * weight
                ).astype(jnp.bfloat16)
                weighted[row * stride + length:(row + 1) * stride, :] = (
                    2.0 * s_re * s_im * weight
                ).astype(jnp.bfloat16)
        result = dot(inverse[...], weighted[...]) * length ** -0.5
        leaving[part] = result.reshape(groups, 2 * share, order).astype(jnp.bfloat16)
        for peer in peers:
            back(part, peer, me).start()
        own = pltpu.make_async_copy(leaving.at[part, me], out_hbm.at[me, part], own_sem.at[1, part])
        own.start()
        returns.append(own)

    for part in range(parts):
        for peer in peers:
            go(part, peer, me).wait_send()

    @pl.when(section < sections - 1)
    def _():
        for piece in range(pieces):
            hop(piece, section + 1).wait_send()

    for part in range(parts):
        returns[part].wait()
        for peer in peers:
            back(part, peer, me).wait_send()
        for peer in peers:
            back(part, peer, peer).wait_recv()


def local(lesser_in, retarded, coupling, interaction):
    order = coupling.shape[-1]
    groups = lax.axis_size("energy")
    sections = lax.axis_size("space")
    length = interaction.shape[1]
    rows = order // groups
    pieces = 2
    parts = 2 if rows % 16 == 0 else 1
    share = rows // parts
    assert lesser_in.shape[0] == 1 and coupling.shape[0] == 1
    forward = jnp.asarray(forward_matrix(groups, length, share))
    inverse = jnp.asarray(inverse_matrix(groups, length, share))
    low, wide = jnp.bfloat16, jnp.float32
    dma = pltpu.SemaphoreType.DMA
    returned = pl.pallas_call(
        functools.partial(kernel, sections, groups, rows, length, pieces, parts),
        out_shape=jax.ShapeDtypeStruct((groups, parts, 2 * share, order), low),
        in_specs=[ANY] * 6,
        out_specs=ANY,
        scratch_shapes=[
            pltpu.VMEM((2, order, order), low),
            pltpu.VMEM((2, order, order), low),
            pltpu.VMEM((2, order, order), low),
            pltpu.VMEM(interaction.shape[1:], low),
            pltpu.VMEM(forward.shape, low),
            pltpu.VMEM(inverse.shape, low),
            pltpu.VMEM((2, order, order), wide),
            pltpu.VMEM((2, order, order), low),
            pltpu.VMEM((2, order, order), low),
            pltpu.VMEM((2, order, order), low),
            pltpu.VMEM((parts, groups, 2 * share, order), low),
            pltpu.VMEM((parts, groups, 2 * share, order), low),
            pltpu.VMEM((share * 2 * length, order), low),
            pltpu.VMEM((parts, groups, 2 * share, order), low),
            dma((6,)),
            dma((pieces,)),
            dma((pieces,)),
            dma((parts, groups)),
            dma((parts, groups)),
            dma((parts, groups)),
            dma((parts, groups)),
            dma((2, parts)),
        ],
        compiler_params=pltpu.CompilerParams(
            collective_id=0, has_side_effects=True
        ),
    )(lesser_in, retarded, coupling, interaction, forward, inverse)
    returned = returned.reshape(groups, parts, 2, share, order).transpose(2, 0, 1, 3, 4)
    return returned.reshape(1, 1, 2, order, order)


def solution(mesh):
    in_specs = (
        P("energy", "space", None, None, None),
        P("energy", "space", None, None, None),
        P("space", None, None, None),
        P("space", None, "energy"),
    )
    out_specs = P("energy", "space", None, None, None)
    return jax.shard_map(local, mesh=mesh, in_specs=in_specs, out_specs=out_specs, check_vma=False)
```

```python
import functools
import math

import jax
import jax.numpy as jnp
import numpy as np
from jax import lax
from jax.experimental import pallas as pl
from jax.experimental.pallas import tpu as pltpu
from jax.sharding import PartitionSpec as P

MESH = pl.DeviceIdType.MESH
ANY = pl.BlockSpec(memory_space=pl.ANY)


def phase_parts(row_count, column_count, length):
    residue = np.arange(row_count)[:, None] * np.arange(column_count)[None, :] % length
    phase = residue * (2.0 * math.pi / length)
    return np.cos(phase), np.sin(phase)


def forward_matrix(energy_count, length, rows):
    cosine, sine = phase_parts(length, energy_count, length)
    small = np.array([[cosine, sine], [-sine, cosine]])
    full = np.einsum("pqfe,rs->rpfeqs", small, np.eye(rows))
    return full.reshape(rows * 2 * length, energy_count * 2 * rows).astype(jnp.bfloat16)


def inverse_matrix(energy_count, length, rows):
    cosine, sine = phase_parts(energy_count, length, length)
    small = np.array([[cosine, -sine], [sine, cosine]])
    full = np.einsum("pqef,rs->eprsqf", small, np.eye(rows))
    return full.reshape(energy_count * 2 * rows, rows * 2 * length).astype(jnp.bfloat16)


def dot(left, right):
    return jnp.dot(left, right, preferred_element_type=jnp.float32)


def dot_t(left, right):
    return lax.dot_general(
        left, right, (((1,), (1,)), ((), ())), preferred_element_type=jnp.float32
    )


def kernel(
    sections, groups, rows, length, pieces, parts,
    lesser_hbm, retarded_hbm, coupling_hbm, interaction_hbm, forward_hbm, inverse_hbm,
    out_hbm,
    lesser, retarded, coupling, interaction, forward, inverse,
    total, maps, green, before, homing, homed, weighted, leaving,
    load_sem, hop_send, hop_recv, go_send, go_recv, back_send, back_recv, own_sem,
):
    section = lax.axis_index("space")
    me = lax.axis_index("energy")
    order = green.shape[-1]
    width = order // pieces

    barrier = pltpu.get_barrier_semaphore()
    for step in range(1, groups):
        peer = lax.rem(me + step, groups)
        pl.semaphore_signal(barrier, inc=1, device_id={"energy": peer}, device_id_type=MESH)

    @pl.when(section > 0)
    def _():
        pl.semaphore_signal(barrier, inc=1, device_id={"space": section - 1}, device_id_type=MESH)

    @pl.when(section < sections - 1)
    def _():
        pl.semaphore_signal(barrier, inc=1, device_id={"space": section + 1}, device_id_type=MESH)

    loads = []
    for at, (source, target) in enumerate((
        (retarded_hbm.at[0, 0], retarded),
        (lesser_hbm.at[0, 0], lesser),
        (coupling_hbm.at[0], coupling),
        (interaction_hbm.at[0], interaction),
        (forward_hbm, forward),
        (inverse_hbm, inverse),
    )):
        load = pltpu.make_async_copy(source, target, load_sem.at[at])
        load.start()
        loads.append(load)

    loads[0].wait()
    loads[1].wait()
    r_re, r_im = retarded[0], retarded[1]
    l_re, l_im = lesser[0], lesser[1]
    half_re = (dot(r_re, l_re) - dot(r_im, l_im)).astype(jnp.bfloat16)
    half_im = (dot(r_re, l_im) + dot(r_im, l_re)).astype(jnp.bfloat16)
    total[0] = dot_t(half_re, r_re) + dot_t(half_im, r_im)
    total[1] = dot_t(half_im, r_re) - dot_t(half_re, r_im)

    pl.semaphore_wait(
        barrier,
        groups - 1 + jnp.where(section > 0, 1, 0) + jnp.where(section < sections - 1, 1, 0),
    )
    loads[2].wait()

    def hop(piece, target):
        columns = pl.ds(piece * width, width)
        return pltpu.make_async_remote_copy(
            src_ref=green.at[:, :, columns],
            dst_ref=before.at[:, :, columns],
            send_sem=hop_send.at[piece],
            recv_sem=hop_recv.at[piece],
            device_id={"space": target},
            device_id_type=MESH,
        )

    @pl.when(section > 0)
    def _():
        c_re, c_im = coupling[0], coupling[1]
        maps[0] = (dot(r_re, c_re) - dot(r_im, c_im)).astype(jnp.bfloat16)
        maps[1] = (dot(r_re, c_im) + dot(r_im, c_re)).astype(jnp.bfloat16)
        for piece in range(pieces):
            hop(piece, section - 1).wait_recv()
            part = slice(piece * width, (piece + 1) * width)
            b_re, b_im = before[0, :, part], before[1, :, part]
            m_re, m_im = maps[0], maps[1]
            k_re = (dot(m_re, b_re) - dot(m_im, b_im)).astype(jnp.bfloat16)
            k_im = (dot(m_re, b_im) + dot(m_im, b_re)).astype(jnp.bfloat16)
            n_re, n_im = maps[0, :, part], maps[1, :, part]
            total[0] += dot_t(k_re, n_re) + dot_t(k_im, n_im)
            total[1] += dot_t(k_im, n_re) - dot_t(k_re, n_im)

    @pl.when(section < sections - 1)
    def _():
        green[...] = total[...].astype(jnp.bfloat16)
        for piece in range(pieces):
            hop(piece, section + 1).start()

    share = rows // parts
    for part in range(parts):
        homing[part] = jnp.concatenate(
            [
                total[side].reshape(groups, parts, share, order)[:, part]
                for side in range(2)
            ],
            axis=1,
        ).astype(jnp.bfloat16)

    def go(part, peer, slot):
        return pltpu.make_async_remote_copy(
            src_ref=homing.at[part, peer],
            dst_ref=homed.at[part, slot],
            send_sem=go_send.at[part, peer],
            recv_sem=go_recv.at[part, slot],
            device_id={"energy": peer},
            device_id_type=MESH,
        )

    def back(part, peer, slot):
        return pltpu.make_async_remote_copy(
            src_ref=leaving.at[part, peer],
            dst_ref=out_hbm.at[slot, part],
            send_sem=back_send.at[part, peer],
            recv_sem=back_recv.at[part, slot],
            device_id={"energy": peer},
            device_id_type=MESH,
        )

    far_first = sorted(range(1, groups), key=lambda step: -min(step, groups - step))
    peers = [lax.rem(me + step, groups) for step in far_first]
    kept = []
    for part in range(parts):
        for peer in peers:
            go(part, peer, me).start()
        own = pltpu.make_async_copy(homing.at[part, me], homed.at[part, me], own_sem.at[0, part])
        own.start()
        kept.append(own)
    for load in loads[3:]:
        load.wait()

    stride = 2 * length
    chunk = max(1, order // stride)
    returns = []
    for part in range(parts):
        kept[part].wait()
        for peer in peers:
            go(part, peer, peer).wait_recv()
        entries = homed[part]
        if 2 * share % 16:
            entries = entries.astype(jnp.float32)
        entries = entries.reshape(groups * 2 * share, order).astype(jnp.bfloat16)
        for first in range(0, share, chunk):
            spectrum = dot(forward[first * stride:(first + chunk) * stride, :], entries)
            spectrum = spectrum * groups ** -0.5
            for at in range(chunk):
                row = first + at
                s_re = spectrum[at * stride:at * stride + length]
                s_im = spectrum[at * stride + length:(at + 1) * stride]
                entry = (part * share + row) * order
                weight = interaction[:, entry:entry + order].astype(jnp.float32)
                weighted[row * stride:row * stride + length, :] = (
                    (s_re * s_re - s_im * s_im) * weight
                ).astype(jnp.bfloat16)
                weighted[row * stride + length:(row + 1) * stride, :] = (
                    2.0 * s_re * s_im * weight
                ).astype(jnp.bfloat16)
        result = dot(inverse[...], weighted[...]) * length ** -0.5
        leaving[part] = result.reshape(groups, 2 * share, order).astype(jnp.bfloat16)
        for peer in peers:
            back(part, peer, me).start()
        own = pltpu.make_async_copy(leaving.at[part, me], out_hbm.at[me, part], own_sem.at[1, part])
        own.start()
        returns.append(own)

    for part in range(parts):
        for peer in peers:
            go(part, peer, me).wait_send()

    @pl.when(section < sections - 1)
    def _():
        for piece in range(pieces):
            hop(piece, section + 1).wait_send()

    for part in range(parts):
        returns[part].wait()
        for peer in peers:
            back(part, peer, me).wait_send()
        for peer in peers:
            back(part, peer, peer).wait_recv()


def local(lesser_in, retarded, coupling, interaction):
    order = coupling.shape[-1]
    groups = lax.axis_size("energy")
    sections = lax.axis_size("space")
    length = interaction.shape[1]
    rows = order // groups
    pieces = 2
    parts = 2 if rows % 16 == 0 else 1
    share = rows // parts
    assert lesser_in.shape[0] == 1 and coupling.shape[0] == 1
    forward = jnp.asarray(forward_matrix(groups, length, share))
    inverse = jnp.asarray(inverse_matrix(groups, length, share))
    low, wide = jnp.bfloat16, jnp.float32
    dma = pltpu.SemaphoreType.DMA
    returned = pl.pallas_call(
        functools.partial(kernel, sections, groups, rows, length, pieces, parts),
        out_shape=jax.ShapeDtypeStruct((groups, parts, 2 * share, order), low),
        in_specs=[ANY] * 6,
        out_specs=ANY,
        scratch_shapes=[
            pltpu.VMEM((2, order, order), low),
            pltpu.VMEM((2, order, order), low),
            pltpu.VMEM((2, order, order), low),
            pltpu.VMEM(interaction.shape[1:], low),
            pltpu.VMEM(forward.shape, low),
            pltpu.VMEM(inverse.shape, low),
            pltpu.VMEM((2, order, order), wide),
            pltpu.VMEM((2, order, order), low),
            pltpu.VMEM((2, order, order), low),
            pltpu.VMEM((2, order, order), low),
            pltpu.VMEM((parts, groups, 2 * share, order), low),
            pltpu.VMEM((parts, groups, 2 * share, order), low),
            pltpu.VMEM((share * 2 * length, order), low),
            pltpu.VMEM((parts, groups, 2 * share, order), low),
            dma((6,)),
            dma((pieces,)),
            dma((pieces,)),
            dma((parts, groups)),
            dma((parts, groups)),
            dma((parts, groups)),
            dma((parts, groups)),
            dma((2, parts)),
        ],
        compiler_params=pltpu.CompilerParams(
            collective_id=0, has_side_effects=True
        ),
    )(lesser_in, retarded, coupling, interaction, forward, inverse)
    returned = returned.reshape(groups, parts, 2, share, order).transpose(2, 0, 1, 3, 4)
    return returned.reshape(1, 1, 2, order, order)


def solution(mesh):
    in_specs = (
        P("energy", "space", None, None, None),
        P("energy", "space", None, None, None),
        P("space", None, None, None),
        P("space", None, "energy"),
    )
    out_specs = P("energy", "space", None, None, None)
    return jax.shard_map(local, mesh=mesh, in_specs=in_specs, out_specs=out_specs, check_vma=False)
```
